32 devices in a mesh: dp: 8 (over z, x), expert: 4 (over y, core).
Axes of the slice: x: 2, y: 2, z: 4, core: 2. Of those that a mesh axis runs over, the one named last changes fastest.
Arguments:
- acts: bfloat16 [4, 4096, 4096], P('expert', 'dp'), may hold values from -8 to 8
- cotangent: bfloat16 [4, 4096, 14336], P('expert', 'dp'), may hold values from -1 to 1
- basis: bfloat16 [4, 4096, 256], P('expert'), may hold values from -1 to 1, as said below
- first_moment: float32 [4, 256, 14336], P('expert', 'dp'), may hold values from -0.6 to 0.6
- second_moment: float32 [4, 256, 14336], P('expert', 'dp'), may hold values from 0.001 to 0.05
- step_count: int32 [1], replicated, may hold values from 1 to 20
Outputs:
- update: bfloat16 [4, 4096, 14336], P('expert', 'dp')
- new_first: float32 [4, 256, 14336], P('expert', 'dp')
- new_second: float32 [4, 256, 14336], P('expert', 'dp')
The draws below stay inside these ranges and needn't reach their ends.
Inputs may be any that keep to these rules, and one draw needn't show every extreme that they name: Each expert's basis has orthonormal columns.
All inputs are finite; a program needn't handle non-finite values.
Results may differ from the reference program's by a relative error of at most 0.0051.
Values may be sent and summed in bfloat16 or wider, within the bound.
A program may use at most 128 MiB of HBM per device.

```python
import math
import jax
import jax.numpy as jnp

D = 4096
FF = 14336
R = 256
EXPERTS = 4
TOKENS = 4096


def make_basis(key):
    raw = jax.random.normal(jax.random.fold_in(key, 7), (EXPERTS, D, R), jnp.float32)
    ortho, upper = jnp.linalg.qr(raw)
    return ortho


def draw_basis(key, part):
    return make_basis(key).astype(jnp.bfloat16)


def draw_acts(key, part):
    ortho = make_basis(key).astype(jnp.bfloat16).astype(jnp.float32)
    noise = jax.random.normal(jax.random.fold_in(key, 11), (EXPERTS, TOKENS, D), jnp.float32)
    coeffs = jax.random.normal(jax.random.fold_in(key, 13), (EXPERTS, TOKENS, R), jnp.float32)
    ranks = jnp.arange(R, dtype=jnp.float32) / R
    spread = 0.5 * jnp.power(jnp.float32(10.0), ranks)
    along = jnp.einsum('etr,edr->etd', coeffs * spread[None, None, :], ortho)
    return jnp.clip(noise + along, -8.0, 8.0).astype(jnp.bfloat16)


def draw_cotangent(key, part):
    rises = jnp.arange(TOKENS, dtype=jnp.float32) / TOKENS
    base = jax.random.truncated_normal(key, -4.0, 4.0, (EXPERTS, TOKENS, FF), jnp.float32)
    scales = jnp.power(jnp.float32(3.0), rises)
    values = base * scales[None, :, None] / jnp.sqrt(jnp.float32(TOKENS))
    return jnp.clip(values, -1.0, 1.0).astype(jnp.bfloat16)


def levels(own_key, shape, pieces, least, high):
    def one(position, blocks):
        heights = jax.random.uniform(jax.random.fold_in(jax.random.fold_in(own_key, 6), position), (blocks,), jnp.float32, least / len(pieces), high / len(pieces))
        return jnp.repeat(jnp.exp(heights), shape[position] // blocks).reshape((-1,) + (1,) * (len(shape) - position - 1))

    factor_of = one(*pieces[0])
    for cut in pieces[1:]:
        factor_of = factor_of * one(*cut)
    return factor_of


def gaussian(key, extent, width, most, pieces=(), kind=jnp.bfloat16):
    result = width * jax.random.normal(key, extent, jnp.float32)
    if pieces:
        result = result * levels(key, extent, pieces, -0.22, 0.18)
    return jnp.clip(result, -most, most).astype(kind)


def setup_inputs(seed: int = 0) -> dict:
    seeds = jax.random.split(jax.random.key(seed), 7)
    acts = draw_acts(jax.random.fold_in(seeds[6], 71), 0)
    cotangent = draw_cotangent(jax.random.fold_in(seeds[6], 71), 0)
    basis = draw_basis(jax.random.fold_in(seeds[6], 71), 0)
    first_moment = gaussian(seeds[3], (EXPERTS, R, FF), 0.1, 0.6, ((0, 4), (1, 8)), jnp.float32)
    second_moment = jnp.clip(jnp.exp(math.log(0.05) - 3.912023 * jax.random.uniform(seeds[4], (EXPERTS, R, FF), jnp.float32) ** levels(seeds[4], (EXPERTS, R, FF), ((0, 4), (1, 8)), -0.2, 0.2)), 0.001, 0.05)
    step_count = jax.random.randint(seeds[5], (1,), 1, 21).astype(jnp.int32)
    return dict(acts=acts, cotangent=cotangent, basis=basis, first_moment=first_moment, second_moment=second_moment, step_count=step_count)


def reference(acts, cotangent, basis, first_moment, second_moment, step_count):
    count = acts.shape[0]
    sums_list = []
    for index in range(count):
        reduced = jnp.dot(acts[index].astype(jnp.float32), basis[index].astype(jnp.float32), preferred_element_type=jnp.float32).astype(jnp.bfloat16)
        sums_list.append(jnp.dot(reduced.T.astype(jnp.float32), cotangent[index].astype(jnp.float32), preferred_element_type=jnp.float32))
    sums = jnp.stack(sums_list)
    total = jnp.sum(sums * sums)
    limit = 0.25 * jnp.sqrt(jnp.float32(count * R * FF))
    factor = jnp.minimum(jnp.float32(1.0), limit / jnp.sqrt(total + 1e-06))
    grad = sums * factor
    new_first = 0.9 * first_moment + 0.1 * grad
    new_second = 0.999 * second_moment + 0.001 * grad * grad
    steps = step_count[0].astype(jnp.float32)
    corr_one = 1.0 - jnp.power(jnp.float32(0.9), steps)
    corr_two = 1.0 - jnp.power(jnp.float32(0.999), steps)
    normed = (new_first / corr_one / (jnp.sqrt(new_second / corr_two) + 1e-08)).astype(jnp.bfloat16)
    updates = []
    for index in range(count):
        updates.append((0.25 * jnp.dot(basis[index].astype(jnp.float32), normed[index].astype(jnp.float32), preferred_element_type=jnp.float32)).astype(jnp.bfloat16))
    return (jnp.stack(updates), new_first, new_second)
```

```python
import jax
import jax.numpy as jnp
from jax import lax
from jax.sharding import PartitionSpec as P

CHUNKS = 4
LANES = 128


def swap(value, axis, size, bit):
    return lax.ppermute(value, axis, [(i, i ^ bit) for i in range(size)])


def bits_of(size):
    bits = []
    while 1 << len(bits) < size:
        bits.append(1 << len(bits))
    return bits


def orders_of(size):
    bits = bits_of(size)
    other = [bits[1], bits[0]] + bits[2:] if len(bits) > 1 else bits
    return [other] + [bits] * (CHUNKS - 1)


def cuts_of(columns):
    tiles = columns // LANES
    edges = [LANES * (tiles * k // CHUNKS) for k in range(CHUNKS)] + [columns]
    return list(zip(edges[:-1], edges[1:]))


def pick(blocks, slots):
    return jnp.concatenate([blocks[s] for s in slots], axis=0)


def halve_start(reduced, cotangent, order):
    size = reduced.shape[0]
    bit = order[0]
    away = [i for i in range(size) if i & bit]
    kept = [i for i in range(size) if not i & bit]
    sent = jnp.dot(pick(reduced, away), cotangent, preferred_element_type=jnp.float32)
    moved = swap(sent.astype(jnp.bfloat16), "dp", size, bit)
    return kept, moved


def halve_rest(reduced, cotangent, order, kept, moved):
    size, rows, _ = reduced.shape
    own = jnp.dot(pick(reduced, kept), cotangent, preferred_element_type=jnp.float32)
    held = own + moved.astype(jnp.float32)
    for bit in order[1:]:
        part = {i: held[n * rows : (n + 1) * rows] for n, i in enumerate(kept)}
        away = [i for i in kept if i & bit]
        kept = [i for i in kept if not i & bit]
        moved = swap(pick(part, away).astype(jnp.bfloat16), "dp", size, bit)
        held = pick(part, kept) + moved.astype(jnp.float32)
    return held


def double(own, order, size):
    slots, pieces = [[0]], [own]
    for bit in reversed(order):
        slots = slots + [[i ^ bit for i in s] for s in slots]
        pieces = pieces + [swap(p, "dp", size, bit) for p in pieces]
        if size > 8:
            slots, pieces = [sum(slots, [])], [jnp.concatenate(pieces, axis=0)]
    return sum(slots, []), jnp.concatenate(pieces, axis=0)


def local(acts, cotangent, basis, first_moment, second_moment, step_count):
    size = lax.axis_size("dp")
    experts = lax.axis_size("expert")
    me = lax.axis_index("dp")
    acts, cotangent, basis = acts[0], cotangent[0], basis[0]
    width, rank = basis.shape
    columns = cotangent.shape[1]
    rows = rank // size
    orders, cuts = orders_of(size), cuts_of(columns)
    ranks = me ^ jnp.arange(size)

    reduced = lax.dot_general(basis, acts, (((0,), (1,)), ((), ())), preferred_element_type=jnp.float32)
    reduced = reduced.astype(jnp.bfloat16).reshape(size, rows, -1)
    reduced = jnp.take(reduced, ranks, axis=0)
    pieces = [cotangent[:, lo:hi] for lo, hi in cuts]
    begun = [halve_start(reduced, piece, order) for piece, order in zip(pieces, orders)]
    sums = [
        halve_rest(reduced, piece, order, kept, moved)
        for piece, order, (kept, moved) in zip(pieces, orders, begun)
    ]
    sums = jnp.concatenate(sums, axis=1)

    total = jnp.full((8, LANES), jnp.sum(sums * sums))
    for bit in bits_of(size):
        total = total + swap(total, "dp", size, bit)
    for bit in bits_of(experts):
        total = total + swap(total, "expert", experts, bit)
    total = total[0, 0]
    limit = 0.25 * jnp.sqrt(jnp.float32(experts * rank * columns))
    factor = jnp.minimum(jnp.float32(1.0), limit / jnp.sqrt(total + 1e-06))
    grad = sums * factor
    new_first = 0.9 * first_moment[0] + 0.1 * grad
    new_second = 0.999 * second_moment[0] + 0.001 * grad * grad
    steps = step_count[0].astype(jnp.float32)
    corr_one = 1.0 - jnp.power(jnp.float32(0.9), steps)
    corr_two = 1.0 - jnp.power(jnp.float32(0.999), steps)
    normed = (new_first / corr_one / (jnp.sqrt(new_second / corr_two) + 1e-08)).astype(jnp.bfloat16)

    width_rows = width // size
    basis_rows = lax.dynamic_slice_in_dim(basis, me * width_rows, width_rows, 0)
    basis_rows = basis_rows.reshape(width_rows, size, rows)
    update = jnp.zeros((width_rows, columns), jnp.bfloat16)
    for (lo, hi), order in zip(cuts, orders):
        slots, gathered = double(normed[:, lo:hi], order, size)
        left = jnp.take(basis_rows, me ^ jnp.array(slots), axis=1).reshape(width_rows, rank)
        product = jnp.dot(left, gathered, preferred_element_type=jnp.float32)
        update = update.at[:, lo:hi].set((0.25 * product).astype(jnp.bfloat16))
    return (update[None], new_first[None], new_second[None])


def solution(mesh):
    in_specs = (
        P("expert", "dp", None),
        P("expert", "dp", None),
        P("expert", None, None),
        P("expert", "dp", None),
        P("expert", "dp", None),
        P(),
    )
    out_specs = (P("expert", "dp", None), P("expert", "dp", None), P("expert", "dp", None))
    return jax.shard_map(local, mesh=mesh, in_specs=in_specs, out_specs=out_specs, check_vma=False)
```

```python
import jax
import jax.numpy as jnp
from jax import lax
from jax.sharding import PartitionSpec as P

CHUNKS = 4
LANES = 128


def swap(value, axis, size, bit):
    return lax.ppermute(value, axis, [(i, i ^ bit) for i in range(size)])


def bits_of(size):
    bits = []
    while 1 << len(bits) < size:
        bits.append(1 << len(bits))
    return bits


def spread_sum(value, axis, size):
    bits = bits_of(size)
    for first in range(0, len(bits), 3):
        span = 1 << len(bits[first : first + 3])
        moved = [swap(value, axis, size, n * bits[first]) for n in range(1, span)]
        value = sum(moved, value)
    return value


def orders_of(size):
    bits = bits_of(size)
    other = [bits[1], bits[0]] + bits[2:] if len(bits) > 1 else bits
    halving = [other if k % 2 else bits for k in range(CHUNKS)]
    doubling = [other if k == 0 else bits for k in range(CHUNKS)]
    return halving, doubling


def cuts_of(columns):
    tiles = columns // LANES
    edges = [LANES * (tiles * k // CHUNKS) for k in range(CHUNKS)] + [columns]
    return list(zip(edges[:-1], edges[1:]))


def pick(blocks, slots):
    return jnp.concatenate([blocks[s] for s in slots], axis=0)


def halve_start(reduced, cotangent, order):
    size = reduced.shape[0]
    bit = order[0]
    away = [i for i in range(size) if i & bit]
    kept = [i for i in range(size) if not i & bit]
    sent = jnp.dot(pick(reduced, away), cotangent, preferred_element_type=jnp.float32)
    moved = swap(sent.astype(jnp.bfloat16), "dp", size, bit)
    return kept, moved


def halve_rest(reduced, cotangent, order, kept, moved):
    size, rows, _ = reduced.shape
    own = jnp.dot(pick(reduced, kept), cotangent, preferred_element_type=jnp.float32)
    held = own + moved.astype(jnp.float32)
    for bit in order[1:]:
        part = {i: held[n * rows : (n + 1) * rows] for n, i in enumerate(kept)}
        away = [i for i in kept if i & bit]
        kept = [i for i in kept if not i & bit]
        moved = swap(pick(part, away).astype(jnp.bfloat16), "dp", size, bit)
        held = pick(part, kept) + moved.astype(jnp.float32)
    return held


def double(own, order, size):
    rows = own.shape[0]
    slots, pieces = [[0]], [own]
    for bit in reversed(order):
        slots = slots + [[i ^ bit for i in s] for s in slots]
        pieces = pieces + [swap(p, "dp", size, bit) for p in pieces]
        if size > 8:
            slots, pieces = [sum(slots, [])], [jnp.concatenate(pieces, axis=0)]
    blocks = {
        slot: piece[n * rows : (n + 1) * rows] for s, piece in zip(slots, pieces) for n, slot in enumerate(s)
    }
    return pick(blocks, range(size))


def local(acts, cotangent, basis, first_moment, second_moment, step_count):
    size = lax.axis_size("dp")
    experts = lax.axis_size("expert")
    me = lax.axis_index("dp")
    acts, cotangent, basis = acts[0], cotangent[0], basis[0]
    width, rank = basis.shape
    columns = cotangent.shape[1]
    rows = rank // size
    (halving, doubling), cuts = orders_of(size), cuts_of(columns)
    ranks = me ^ jnp.arange(size)

    reduced = lax.dot_general(basis, acts, (((0,), (1,)), ((), ())), preferred_element_type=jnp.float32)
    reduced = reduced.astype(jnp.bfloat16).reshape(size, rows, -1)
    reduced = jnp.take(reduced, ranks, axis=0, mode="clip")
    pieces = [cotangent[:, lo:hi] for lo, hi in cuts]
    begun = [halve_start(reduced, piece, order) for piece, order in zip(pieces, halving)]
    sums = [
        halve_rest(reduced, piece, order, kept, moved)
        for piece, order, (kept, moved) in zip(pieces, halving, begun)
    ]
    sums = jnp.concatenate(sums, axis=1)

    total = jnp.full((8, LANES), jnp.sum(sums * sums))
    total = spread_sum(spread_sum(total, "dp", size), "expert", experts)
    total = total[0, 0]
    limit = 0.25 * jnp.sqrt(jnp.float32(experts * rank * columns))
    factor = jnp.minimum(jnp.float32(1.0), limit / jnp.sqrt(total + 1e-06))
    grad = sums * factor
    new_first = 0.9 * first_moment[0] + 0.1 * grad
    new_second = 0.999 * second_moment[0] + 0.001 * grad * grad
    steps = step_count[0].astype(jnp.float32)
    corr_one = 1.0 - jnp.power(jnp.float32(0.9), steps)
    corr_two = 1.0 - jnp.power(jnp.float32(0.999), steps)
    normed = (new_first / corr_one / (jnp.sqrt(new_second / corr_two) + 1e-08)).astype(jnp.bfloat16)

    width_rows = width // size
    basis_rows = lax.dynamic_slice_in_dim(basis, me * width_rows, width_rows, 0)
    left = jnp.take(basis_rows.reshape(width_rows, size, rows), ranks, axis=1, mode="clip")
    left = left.reshape(width_rows, rank)
    gathered = [double(normed[:, lo:hi], order, size) for (lo, hi), order in zip(cuts, doubling)]
    gathered = jnp.concatenate(gathered, axis=1)
    product = jnp.dot(left, gathered, preferred_element_type=jnp.float32)
    update = (0.25 * product).astype(jnp.bfloat16)
    return (update[None], new_first[None], new_second[None])


def solution(mesh):
    in_specs = (
        P("expert", "dp", None),
        P("expert", "dp", None),
        P("expert", None, None),
        P("expert", "dp", None),
        P("expert", "dp", None),
        P(),
    )
    out_specs = (P("expert", "dp", None), P("expert", "dp", None), P("expert", "dp", None))
    return jax.shard_map(local, mesh=mesh, in_specs=in_specs, out_specs=out_specs, check_vma=False)
```
